32 devices in a mesh: row: 4 (over y, core), col: 8 (over z, x).
Axes of the slice: x: 2, y: 2, z: 4, core: 2. Of those that a mesh axis runs over, the one named last changes fastest.
Arguments:
- density: float32 [4096, 32768], P('row', 'col'), may hold values from 0 to 1
- design_mask: int32 [32, 256], P('row', 'col'), may hold values 0 or 1
- rebalance: int32 [8192], replicated, may hold values from 0 to 8191, as said below
Outputs:
- balanced: bfloat16 [8192, 128, 128], P(('row', 'col'))
- constraint: float32 [], replicated
The draws below stay inside these ranges and needn't reach their ends.
Inputs may be any that keep to these rules, and one draw needn't show every extreme that they name: `rebalance`: A permutation of the 8192 block numbers. Of the blocks that one device holds, the ones that land among one device's output blocks number exactly 8 or none.
All inputs are finite; a program needn't handle non-finite values. No bound on the sum of `design_mask` on one device may be relied on, other than what follows from the above.
Results may differ from the reference program's by a relative error of at most 0.001.
Values may be sent and summed in bfloat16 or wider, within the bound.
No kernel may reach another device: no remote copies, remote signals or barrier semaphores. Data moves between devices by JAX's collectives and lax.ppermute only.
A program may use at most 192 MiB of HBM per device.

```python
import jax
import jax.numpy as jnp
from jax import lax

BS = 128
RADIUS = 16
KR = 8
KC = 32
BLOCKS_DEV = 256
CAP = 8
NX = 4096
NY = 32768
NBLK = 8192
N_ROW = 4
N_COL = 8


def draw_rebalance(key, part):
    device_count = N_ROW * N_COL
    group_count = BLOCKS_DEV // CAP
    base = jax.random.fold_in(key, 11)
    key_order, key_offset, key_source, key_target = jax.random.split(base, 4)
    order = jax.random.permutation(key_order, device_count).astype(jnp.int32)
    inverse = jnp.argsort(order).astype(jnp.int32)
    offsets = jax.random.permutation(key_offset, device_count)[:group_count].astype(jnp.int32)
    source_shuffle = jax.vmap(lambda sub: jax.random.permutation(sub, BLOCKS_DEV))(jax.random.split(key_source, device_count)).astype(jnp.int32)
    target_shuffle = jax.vmap(lambda sub: jax.random.permutation(sub, BLOCKS_DEV))(jax.random.split(key_target, device_count)).astype(jnp.int32)
    positions = jnp.arange(NBLK, dtype=jnp.int32)
    target_dev = positions // BLOCKS_DEV
    target_slot = positions % BLOCKS_DEV
    raw_slot = target_shuffle[target_dev, target_slot]
    group = raw_slot // CAP
    within = raw_slot % CAP
    source_dev = (inverse[target_dev] - offsets[group]) % device_count
    local_block = source_shuffle[source_dev, group * CAP + within]
    source_row = source_dev // N_COL
    source_col = source_dev % N_COL
    block_row = source_row * KR + local_block // KC
    block_col = source_col * KC + local_block % KC
    return (block_row * (KC * N_COL) + block_col).astype(jnp.int32)


def set_ends(entries, own_key, smallest, largest):
    place = [jax.random.randint(jax.random.fold_in(own_key, axis), (), 0, length) for axis, length in enumerate(entries.shape)]
    longest = entries.shape.index(max(entries.shape))
    next_to = place[:longest] + [(place[longest] + 1) % entries.shape[longest]] + place[longest + 1:]
    return entries.at[tuple(place)].set(smallest).at[tuple(next_to)].set(largest)


def levels(key, shape, cuts, smallest, high):
    factor_of = 1.0
    for axis_at, shards_of in cuts:
        heights = jax.random.uniform(jax.random.fold_in(jax.random.fold_in(key, 6), axis_at), (shards_of,), jnp.float32, smallest / len(cuts), high / len(cuts))
        factor_of = factor_of * jnp.repeat(jnp.exp(heights), shape[axis_at] // shards_of).reshape((-1,) + (1,) * (len(shape) - 1 - axis_at))
    return factor_of


def setup_inputs(seed: int = 0) -> dict:
    key_list = jax.random.split(jax.random.key(seed), 4)
    return {
        "density": jnp.clip(1.0 * jax.random.uniform(key_list[0], (NX, NY), jnp.float32) ** levels(key_list[0], (NX, NY), ((0, 4), (1, 8)), -0.2, 0.2), 0.0, 1.0),
        "design_mask": set_ends((jax.random.randint(key_list[1], (NX // BS, NY // BS), 0, 4) < 3).astype(jnp.int32), jax.random.fold_in(key_list[1], 1), 0, 1),
        "rebalance": draw_rebalance(jax.random.fold_in(key_list[3], 71), 0),
    }


SHARPNESS = 32.0
THRESHOLD = 0.5
VOLUME_TARGET = 0.4


def filter_taps():
    sigma = RADIUS / 4.0
    offsets = jnp.arange(2 * RADIUS + 1, dtype=jnp.float32) - RADIUS
    raw_taps = jnp.exp(-offsets * offsets / (2.0 * sigma * sigma))
    return raw_taps / jnp.sum(raw_taps)


def smooth(field, weights, axis):
    length = field.shape[axis]
    widths = [(0, 0), (0, 0)]
    widths[axis] = (RADIUS, RADIUS)
    padded = jnp.pad(field, widths)
    total = jnp.zeros_like(field)
    for offset in range(2 * RADIUS + 1):
        total = total + weights[offset] * lax.slice_in_dim(padded, offset, offset + length, axis=axis)
    return total


def reference(density, design_mask, rebalance):
    weights = filter_taps()
    along_rows = smooth(density, weights, 0)
    filtered = smooth(along_rows, weights, 1)
    cell_mask = jnp.repeat(jnp.repeat(design_mask, BS, 0), BS, 1).astype(jnp.float32)
    lower = jnp.tanh(SHARPNESS * THRESHOLD)
    upper = jnp.tanh(SHARPNESS * (1.0 - THRESHOLD))
    projected = cell_mask * (lower + jnp.tanh(SHARPNESS * (filtered - THRESHOLD))) / (lower + upper)
    constraint = jnp.sum(projected) / (NX * NY) / VOLUME_TARGET - 1.0
    block_rows = NX // BS
    block_cols = NY // BS
    tiles = projected.astype(jnp.bfloat16).reshape(block_rows, BS, block_cols, BS)
    tiles = tiles.transpose(0, 2, 1, 3).reshape(block_rows * block_cols, BS, BS)
    balanced = jnp.take(tiles, rebalance.astype(jnp.int32), axis=0)
    return balanced, constraint
```

```python
import functools

import jax
import jax.numpy as jnp
import numpy as np
from jax import lax
from jax.experimental import pallas as pl
from jax.experimental.pallas import tpu as pltpu
from jax.sharding import PartitionSpec as P

BS = 128
RADIUS = 16
PAD = BS + 2 * RADIUS
WIDE = 3 * BS
BUFFERS = 3

SHARPNESS = 32.0
THRESHOLD = 0.5
VOLUME_TARGET = 0.4

AXES = ("row", "col")


def filter_taps():
    sigma = RADIUS / 4.0
    offsets = np.arange(2 * RADIUS + 1, dtype=np.float64) - RADIUS
    raw_taps = np.exp(-offsets * offsets / (2.0 * sigma * sigma))
    return raw_taps / raw_taps.sum()


def split_taps(matrix):
    high = matrix.astype(jnp.bfloat16)
    low = (matrix - high.astype(np.float64)).astype(jnp.bfloat16)
    return high, low


def column_matrix():
    taps = filter_taps()
    source = np.concatenate([np.arange(BS), np.arange(BS)])
    source[BS:BS + RADIUS] += BS
    source[2 * BS - RADIUS:] -= BS
    used = np.ones(2 * BS, bool)
    used[BS + RADIUS:2 * BS - RADIUS] = False
    lag = source[:, None] - np.arange(BS)[None, :] + RADIUS
    inside = (lag >= 0) & (lag <= 2 * RADIUS) & used[:, None]
    matrix = np.where(inside, taps[np.clip(lag, 0, 2 * RADIUS)], 0.0)
    return np.concatenate(split_taps(matrix), axis=1)


def row_matrix():
    taps = filter_taps()
    lag = np.arange(PAD)[None, :] - np.arange(BS)[:, None]
    inside = (lag >= 0) & (lag <= 2 * RADIUS)
    matrix = np.where(inside, taps[np.clip(lag, 0, 2 * RADIUS)], 0.0)
    high, low = split_taps(matrix)
    return np.concatenate([high, high, low], axis=1)


def exchange_order(row_count, col_count):
    device_count = row_count * col_count
    quarter = max(1, col_count // 4)
    long_part = [2, 3, 1] if col_count >= 4 else [1]
    rest = [r * col_count + c for r in range(row_count) for c in range(quarter)]
    far = [long * quarter + other for other in rest for long in long_part]
    near = [other for other in rest if other]
    order = []
    while far or near:
        order, far = order + far[:3], far[3:]
        if near:
            order.append(near.pop(0))
    order = [d for d in order if 0 < d < device_count]
    assert sorted(order) == list(range(1, device_count))
    return order


def with_halo(density):
    rows, cols = density.shape

    def moves(axis):
        up = [(i, i + 1) for i in range(lax.axis_size(axis) - 1)]
        return up, [(j, i) for i, j in up]

    up, down = moves("row")
    top = lax.ppermute(density[rows - RADIUS:], "row", up)
    bottom = lax.ppermute(density[:RADIUS], "row", down)
    up, down = moves("col")

    def strip(start):
        parts = [a[:, start:start + RADIUS].T for a in (top, density, bottom)]
        return jnp.concatenate(parts, axis=1)

    left = lax.ppermute(strip(cols - RADIUS), "col", up)
    right = lax.ppermute(strip(0), "col", down)
    left = jnp.pad(left, ((BS - RADIUS, 0), (0, 0))).T
    right = jnp.pad(right, ((0, BS - RADIUS), (0, 0))).T
    return top, bottom, left, right


def block_tables(rebalance, me, mask_rows, mask_cols, row_count, col_count, capacity):
    device_count = row_count * col_count
    block_count = mask_rows * mask_cols
    wanted = rebalance.reshape(device_count, block_count)
    block_row = lax.div(wanted, mask_cols * col_count)
    block_col = lax.rem(wanted, mask_cols * col_count)
    source = lax.div(block_row, mask_rows) * col_count + lax.div(block_col, mask_cols)
    local = lax.rem(block_row, mask_rows) * mask_cols + lax.rem(block_col, mask_cols)
    slots = jnp.arange(block_count, dtype=jnp.int32)
    devices = jnp.arange(device_count, dtype=jnp.int32)
    mine = lax.dynamic_index_in_dim(source, me, 0, keepdims=True)
    match = jnp.concatenate([source == me, mine == devices[:, None]], axis=0)
    value = jnp.concatenate([local, jnp.broadcast_to(slots, local.shape)], axis=0)
    before = (slots[:, None] < slots[None, :]).astype(jnp.bfloat16)
    rank = jnp.dot(match.astype(jnp.bfloat16), before, preferred_element_type=jnp.float32)
    rank = jnp.where(match, rank.astype(jnp.int32), -1)
    ranks = jnp.arange(capacity, dtype=jnp.int32)
    chosen = rank[:, None, :] == ranks[None, :, None]
    return jnp.sum(jnp.where(chosen, value[:, None, :], 0), axis=2).reshape(-1)


class Meta:
    def __init__(self, device_count, capacity, block_count):
        self.capacity = capacity
        self.send = 0
        self.place = device_count * capacity
        self.mask = 2 * device_count * capacity
        self.order = self.mask + block_count
        self.me = self.order + device_count


def project_kernel(meta_ref, dens, top, bottom, left, right, wcol, wrow, acc_in, *refs,
                   layout, first, count, block_rows, block_cols, has_local):
    capacity = layout.capacity
    outs, acc_out = refs[:count], refs[count]
    buf, fetch_sem, tiles, store_sem = refs[count + 1:]
    me = meta_ref[layout.me]
    pairs = count * capacity // 2

    def block_of(step):
        where = first * capacity + step
        target = me ^ meta_ref[layout.order + lax.div(where, capacity)]
        return meta_ref[layout.send + target * capacity + lax.rem(where, capacity)]

    def fetch(pair, slot):
        for half in range(2):
            block = block_of(2 * pair + half)
            br = lax.div(block, block_cols)
            bc = lax.rem(block, block_cols)
            row0 = pl.multiple_of(br * BS, BS)
            col0 = pl.multiple_of(bc * BS, BS)
            window = buf.at[slot, half]
            sem = fetch_sem.at[slot, half]

            def copy(src, rows, cols):
                pltpu.make_async_copy(src, window.at[pl.ds(*rows), pl.ds(*cols)], sem).start()

            for side_col in range(3):
                if side_col == 0:
                    c_src, c_dst, c_len = col0, BS, 2 * BS
                    c_if = bc == 0
                elif side_col == 1:
                    c_src, c_dst, c_len = pl.multiple_of(col0 - BS, BS), 0, 3 * BS
                    c_if = (bc > 0) & (bc < block_cols - 1)
                else:
                    c_src, c_dst, c_len = pl.multiple_of(col0 - BS, BS), 0, 2 * BS
                    c_if = bc == block_cols - 1

                @pl.when(c_if)
                def _():
                    if side_col == 0:
                        copy(left.at[pl.ds(row0, PAD), :], (0, PAD), (0, BS))
                    if side_col == 2:
                        copy(right.at[pl.ds(row0, PAD), :], (0, PAD), (2 * BS, BS))
                    span = pl.ds(c_src, c_len)

                    @pl.when(br == 0)
                    def _():
                        copy(top.at[:, span], (0, RADIUS), (c_dst, c_len))
                        copy(dens.at[pl.ds(0, PAD - RADIUS), span],
                             (RADIUS, PAD - RADIUS), (c_dst, c_len))

                    @pl.when((br > 0) & (br < block_rows - 1))
                    def _():
                        row1 = pl.multiple_of(row0 - RADIUS, RADIUS)
                        copy(dens.at[pl.ds(row1, PAD), span], (0, PAD), (c_dst, c_len))

                    @pl.when(br == block_rows - 1)
                    def _():
                        last = block_rows * BS - (PAD - RADIUS)
                        copy(dens.at[pl.ds(last, PAD - RADIUS), span],
                             (0, PAD - RADIUS), (c_dst, c_len))
                        copy(bottom.at[:, span], (PAD - RADIUS, RADIUS), (c_dst, c_len))

    acc_out[...] = acc_in[...]
    for ahead in range(min(BUFFERS - 1, pairs)):
        fetch(ahead, ahead)

    lower = float(np.tanh(SHARPNESS * THRESHOLD))
    upper = float(np.tanh(SHARPNESS * (1.0 - THRESHOLD)))
    lane = lax.broadcasted_iota(jnp.int32, (2, PAD, BS), 2)

    @pl.loop(0, pairs)
    def _(pair):
        slot = lax.rem(pair, BUFFERS)

        @pl.when(pair + BUFFERS - 1 < pairs)
        def _():
            fetch(pair + BUFFERS - 1, lax.rem(pair + BUFFERS - 1, BUFFERS))

        for half in range(2):
            pltpu.make_async_copy(dens.at[pl.ds(0, PAD), pl.ds(0, WIDE)],
                                  buf.at[slot, half], fetch_sem.at[slot, half]).wait()
        middle = buf[slot, :, :, BS:2 * BS]
        sides = jnp.where(lane < BS // 2, buf[slot, :, :, 2 * BS:], buf[slot, :, :, :BS])
        x = jnp.concatenate([middle, sides], axis=2).reshape(2 * PAD, 2 * BS)
        x_high = x.astype(jnp.bfloat16)
        x_low = (x - x_high.astype(jnp.float32)).astype(jnp.bfloat16)
        taps = wcol[...]
        both = jnp.dot(x_high, taps, preferred_element_type=jnp.float32)
        y = both[:, :BS] + (both[:, BS:] + jnp.dot(
            x_low, taps[:, :BS], preferred_element_type=jnp.float32))
        y = jnp.concatenate([y[:PAD], y[PAD:]], axis=1)
        y_high = y.astype(jnp.bfloat16)
        y_low = (y - y_high.astype(jnp.float32)).astype(jnp.bfloat16)
        stacked = jnp.concatenate([y_high, y_low, y_high], axis=0)
        filtered = jnp.dot(wrow[...], stacked, preferred_element_type=jnp.float32)
        raised = lower + jnp.tanh(SHARPNESS * (filtered - THRESHOLD))
        for half in range(2):
            step = 2 * pair + half
            keep = meta_ref[layout.mask + block_of(step)].astype(jnp.float32)
            value = raised[:, half * BS:(half + 1) * BS] * (keep * (1.0 / (lower + upper)))
            tiles[step] = value.astype(jnp.bfloat16)
            acc_out[...] += jnp.sum(value.reshape(BS // 8, 8, BS), axis=0)

    stores = []
    for g in range(count):
        if has_local and g == count - 1:
            for r in range(capacity):
                slot = meta_ref[layout.place + me * capacity + r]
                stores.append(pltpu.make_async_copy(
                    tiles.at[g * capacity + r], outs[g].at[slot], store_sem.at[len(stores)]))
        else:
            stores.append(pltpu.make_async_copy(
                tiles.at[pl.ds(g * capacity, capacity)], outs[g], store_sem.at[len(stores)]))
    for store in stores:
        store.start()
    for store in stores:
        store.wait()


def project(meta, fields, acc, *, layout, first, count, block_rows, block_cols, has_local):
    capacity = layout.capacity
    block_count = block_rows * block_cols
    sent = jax.ShapeDtypeStruct((capacity, BS, BS), jnp.bfloat16)
    whole = jax.ShapeDtypeStruct((block_count, BS, BS), jnp.bfloat16)
    shapes = [sent] * count
    if has_local:
        shapes[-1] = whole
    anywhere = pl.BlockSpec(memory_space=pl.ANY)
    vmem = pl.BlockSpec(memory_space=pltpu.VMEM)
    kernel = functools.partial(
        project_kernel, layout=layout, first=first, count=count, block_rows=block_rows,
        block_cols=block_cols, has_local=has_local)
    steps = count * capacity
    results = pl.pallas_call(
        kernel,
        out_shape=tuple(shapes) + (jax.ShapeDtypeStruct((8, BS), jnp.float32),),
        in_specs=[pl.BlockSpec(memory_space=pltpu.SMEM)] + [anywhere] * 5 + [vmem] * 3,
        out_specs=tuple([anywhere] * count + [vmem]),
        scratch_shapes=[
            pltpu.VMEM((BUFFERS, 2, PAD, WIDE), jnp.float32),
            pltpu.SemaphoreType.DMA((BUFFERS, 2)),
            pltpu.VMEM((steps, BS, BS), jnp.bfloat16),
            pltpu.SemaphoreType.DMA((count + capacity,)),
        ],
        cost_estimate=pl.CostEstimate(
            flops=steps * 300_000_000, bytes_accessed=steps * 300_000, transcendentals=0),
        name="project",
    )(meta, *fields, acc)
    return results[:-1], results[-1]


def place_kernel(meta_ref, out_in, *refs, layout, offsets):
    del out_in
    arrived, out, sem = refs[:len(offsets)], refs[len(offsets)], refs[len(offsets) + 1]
    capacity = layout.capacity
    me = meta_ref[layout.me]
    for part, offset in zip(arrived, offsets):
        for r in range(capacity):
            slot = meta_ref[layout.place + (me ^ offset) * capacity + r]
            pltpu.make_async_copy(part.at[r], out.at[slot], sem).start()
    everything = out.at[pl.ds(0, len(offsets) * capacity)]
    pltpu.make_async_copy(everything, everything, sem).wait()


def place(meta, out, arrived, offsets, *, layout):
    anywhere = pl.BlockSpec(memory_space=pl.ANY)
    return pl.pallas_call(
        functools.partial(place_kernel, layout=layout, offsets=tuple(offsets)),
        out_shape=jax.ShapeDtypeStruct(out.shape, out.dtype),
        in_specs=[pl.BlockSpec(memory_space=pltpu.SMEM)] + [anywhere] * (1 + len(offsets)),
        out_specs=anywhere,
        scratch_shapes=[pltpu.SemaphoreType.DMA],
        input_output_aliases={1: 0},
        name="place",
    )(meta, out, *arrived)


def grouped(items, sizes):
    groups = []
    for size in sizes:
        if items:
            groups.append(items[:size])
            items = items[size:]
    return groups


def per_device(density, design_mask, rebalance):
    tile_rows, tile_cols = density.shape
    block_rows, block_cols = design_mask.shape
    block_count = block_rows * block_cols
    row_count = lax.axis_size("row")
    col_count = lax.axis_size("col")
    device_count = row_count * col_count
    capacity = block_count // device_count
    assert capacity * device_count == block_count and capacity % 2 == 0
    assert block_rows > 1 and block_cols > 1
    me = lax.axis_index(AXES)
    order = exchange_order(row_count, col_count)
    layout = Meta(device_count, capacity, block_count)
    top, bottom, left, right = with_halo(density)
    tables = block_tables(
        rebalance, me, block_rows, block_cols, row_count, col_count, capacity)
    meta = jnp.concatenate([
        tables, design_mask.reshape(-1), jnp.array(order + [0], jnp.int32),
        jnp.broadcast_to(me, (8,)).astype(jnp.int32)])
    fields = (density, top, bottom, left, right,
              jnp.asarray(column_matrix()), jnp.asarray(row_matrix()))

    unit = max(1, 8 // capacity)
    sizes = [unit, unit, 2 * unit, 3 * unit] + [4 * unit] * device_count
    groups = grouped(order, sizes)
    groups[-1] = groups[-1] + [0]
    acc = jnp.zeros((8, BS), jnp.float32)
    arrivals, first, out = [], 0, None
    for group in groups:
        sent, acc = project(
            meta, fields, acc, layout=layout, first=first, count=len(group),
            block_rows=block_rows, block_cols=block_cols, has_local=group[-1] == 0)
        for offset, part in zip(group, sent):
            if offset:
                pairs = [(i, i ^ offset) for i in range(device_count)]
                arrivals.append(lax.ppermute(part, AXES, pairs))
            else:
                out = part
        first += len(group)

    tail = [2 * unit, 1 * unit]
    sizes = [4 * unit] * ((len(order) - sum(tail)) // (4 * unit))
    sizes = [len(order) - sum(tail) - sum(sizes)] + sizes + tail
    begin = 0
    for size in sizes:
        if size:
            out = place(meta, out, arrivals[begin:begin + size], order[begin:begin + size],
                        layout=layout)
        begin += size

    total_volume = lax.psum(jnp.sum(acc), AXES)
    grid_cells = float(tile_rows * tile_cols * device_count)
    constraint = total_volume / grid_cells / VOLUME_TARGET - 1.0
    return out, constraint


def solution(mesh):
    return jax.shard_map(
        per_device,
        mesh=mesh,
        in_specs=(P("row", "col"), P("row", "col"), P()),
        out_specs=(P(AXES, None, None), P()),
        check_vma=False,
    )
```

```python
import functools

import jax
import jax.numpy as jnp
import numpy as np
from jax import lax
from jax.experimental import pallas as pl
from jax.experimental.pallas import tpu as pltpu
from jax.sharding import PartitionSpec as P


BS = 128
RADIUS = 16
PAD = BS + 2 * RADIUS
WIDE = 3 * BS
BUFFERS = 4
GROUPS = (2, 4, 8, 8, 10)

SHARPNESS = 32.0
THRESHOLD = 0.5
VOLUME_TARGET = 0.4

AXES = ("row", "col")


def tap_parts():
    sigma = RADIUS / 4.0
    offsets = np.arange(2 * RADIUS + 1, dtype=np.float64) - RADIUS
    raw_taps = np.exp(-offsets * offsets / (2.0 * sigma * sigma))
    taps = raw_taps / raw_taps.sum()
    high = taps.astype(jnp.bfloat16)
    rest = taps - high.astype(np.float64)
    missing = (rest - rest.astype(jnp.bfloat16).astype(np.float64)).sum()
    rest[0] += missing / 2
    rest[-1] += missing / 2
    return high, rest.astype(jnp.bfloat16)


def band_matrices():
    parts = tap_parts()

    def bands(lag, used):
        used = used & (np.abs(lag) <= RADIUS)
        index = np.clip(lag + RADIUS, 0, 2 * RADIUS)
        return [np.where(used, part[index], np.zeros((), part.dtype)) for part in parts]

    lane = np.arange(2 * BS)[:, None]
    source = np.where(lane < 2 * BS - RADIUS, lane, lane - 2 * BS)
    used = (lane < BS + RADIUS) | (lane >= 2 * BS - RADIUS)
    columns = bands(source - np.arange(BS)[None, :], used)
    lag = np.arange(PAD)[None, :] - RADIUS - np.arange(BS)[:, None]
    rows = bands(lag, np.ones_like(lag, bool))
    return (jnp.asarray(np.concatenate(columns, axis=1)),
            jnp.asarray(np.concatenate([rows[0], rows[0], rows[1]], axis=1)))


def exchange_order(row_count, col_count):
    device_count = row_count * col_count
    quarter = max(1, col_count // 4)
    long_part = [2, 3, 1] if col_count >= 4 else [1]
    rest = [r * col_count + c for r in range(row_count) for c in range(quarter)]
    far = [long * quarter + other for other in rest for long in long_part]
    near = [other for other in rest if other]
    order = []
    while far or near:
        order, far = order + far[:3], far[3:]
        if near:
            order.append(near.pop(0))
    order = [d for d in order if 0 < d < device_count]
    assert sorted(order) == list(range(1, device_count))
    return order


def with_halo(density):
    rows, cols = density.shape

    def moves(axis):
        up = [(i, i + 1) for i in range(lax.axis_size(axis) - 1)]
        return up, [(j, i) for i, j in up]

    up, down = moves("row")
    top = lax.ppermute(density[rows - RADIUS:], "row", up)
    bottom = lax.ppermute(density[:RADIUS], "row", down)
    up, down = moves("col")

    def strip(start):
        parts = [a[:, start:start + RADIUS].T for a in (top, density, bottom)]
        return jnp.concatenate(parts, axis=1)

    left = lax.ppermute(strip(cols - RADIUS), "col", up)
    right = lax.ppermute(strip(0), "col", down)
    left = jnp.pad(left, ((BS - RADIUS, 0), (0, 0))).T
    right = jnp.pad(right, ((0, BS - RADIUS), (0, 0))).T
    return top, bottom, left, right


def block_tables(rebalance, me, mask_rows, mask_cols, row_count, col_count, capacity, order):
    device_count = row_count * col_count
    block_count = mask_rows * mask_cols
    wanted = rebalance.reshape(device_count, block_count)
    block_row = lax.div(wanted, mask_cols * col_count)
    block_col = lax.rem(wanted, mask_cols * col_count)
    source = lax.div(block_row, mask_rows) * col_count + lax.div(block_col, mask_cols)
    local = lax.rem(block_row, mask_rows) * mask_cols + lax.rem(block_col, mask_cols)
    slots = jnp.arange(block_count, dtype=jnp.int32)
    devices = jnp.arange(device_count, dtype=jnp.int32)
    mine = lax.dynamic_index_in_dim(source, me, 0, keepdims=True)
    match = jnp.concatenate([source == me, mine == devices[:, None]], axis=0)
    value = jnp.concatenate([local, jnp.broadcast_to(slots, local.shape)], axis=0)
    before = (slots[:, None] < slots[None, :]).astype(jnp.bfloat16)
    rank = jnp.dot(match.astype(jnp.bfloat16), before, preferred_element_type=jnp.float32)
    rank = jnp.where(match, rank.astype(jnp.int32), -1)
    ranks = jnp.arange(capacity, dtype=jnp.int32)
    chosen = rank[:, None, :] == ranks[None, :, None]
    table = jnp.sum(jnp.where(chosen, value[:, None, :], 0), axis=2)
    partner = me ^ jnp.array(order, jnp.int32)
    pick = partner[:, None] == devices[None, :]
    table = table.reshape(2, 1, device_count, capacity)
    return jnp.sum(jnp.where(pick[None, :, :, None], table, 0), axis=2).reshape(-1)


class Meta:
    def __init__(self, device_count, capacity):
        self.capacity = capacity
        self.send = 0
        self.place = device_count * capacity
        self.mask = 2 * device_count * capacity


def split_scalar(index, size):
    if size & (size - 1):
        return lax.div(index, size), lax.rem(index, size)
    return lax.shift_right_logical(index, size.bit_length() - 1), index & (size - 1)


def project_kernel(meta_ref, dens, top, bottom, left, right, wcol, wrow, acc_in, *refs,
                   layout, first, count, block_rows, block_cols, has_local):
    capacity = layout.capacity
    outs, acc_out = refs[:count], refs[count]
    buf, fetch_sem, lines, tiles, store_sem = refs[count + 1:]
    pairs = count * capacity // 2
    begin = layout.send + first * capacity

    def fetch(pair, slot):
        for half in range(2):
            block = meta_ref[begin + 2 * pair + half]
            br, bc = split_scalar(block, block_cols)
            row0 = pl.multiple_of(br * BS, BS)
            col0 = pl.multiple_of(bc * BS, BS)
            window = buf.at[slot, half]
            sem = fetch_sem.at[slot, half]
            inside = ((br > 0) & (br < block_rows - 1)) & ((bc > 0) & (bc < block_cols - 1))

            def copy(src, rows, cols):
                pltpu.make_async_copy(src, window.at[pl.ds(*rows), pl.ds(*cols)], sem).start()

            def rows_of(span, c_dst, c_len):
                @pl.when(br == 0)
                def _():
                    copy(top.at[:, span], (0, RADIUS), (c_dst, c_len))
                    copy(dens.at[pl.ds(0, PAD - RADIUS), span],
                         (RADIUS, PAD - RADIUS), (c_dst, c_len))

                @pl.when((br > 0) & (br < block_rows - 1))
                def _():
                    row1 = pl.multiple_of(row0 - RADIUS, RADIUS)
                    copy(dens.at[pl.ds(row1, PAD), span], (0, PAD), (c_dst, c_len))

                @pl.when(br == block_rows - 1)
                def _():
                    last = block_rows * BS - (PAD - RADIUS)
                    copy(dens.at[pl.ds(last, PAD - RADIUS), span],
                         (0, PAD - RADIUS), (c_dst, c_len))
                    copy(bottom.at[:, span], (PAD - RADIUS, RADIUS), (c_dst, c_len))

            @pl.when(inside)
            def _():
                row1 = pl.multiple_of(row0 - RADIUS, RADIUS)
                col1 = pl.multiple_of(col0 - BS, BS)
                pltpu.make_async_copy(
                    dens.at[pl.ds(row1, PAD), pl.ds(col1, WIDE)], window, sem).start()

            @pl.when(jnp.logical_not(inside))
            def _():
                @pl.when(bc == 0)
                def _():
                    copy(left.at[pl.ds(row0, PAD), :], (0, PAD), (0, BS))
                    rows_of(pl.ds(0, 2 * BS), BS, 2 * BS)

                @pl.when((bc > 0) & (bc < block_cols - 1))
                def _():
                    rows_of(pl.ds(pl.multiple_of(col0 - BS, BS), WIDE), 0, WIDE)

                @pl.when(bc == block_cols - 1)
                def _():
                    copy(right.at[pl.ds(row0, PAD), :], (0, PAD), (2 * BS, BS))
                    rows_of(pl.ds((block_cols - 2) * BS, 2 * BS), 0, 2 * BS)

    lower = float(np.tanh(SHARPNESS * THRESHOLD))
    upper = float(np.tanh(SHARPNESS * (1.0 - THRESHOLD)))

    def along_columns(pair):
        slot = lax.rem(pair, BUFFERS)
        lane = lax.broadcasted_iota(jnp.int32, (PAD, BS), 1)
        taps = wcol[...]
        for half in range(2):
            window = buf.at[slot, half]
            sides = jnp.where(lane < BS // 2, window[:, 2 * BS:], window[:, :BS])
            x = jnp.concatenate([window[:, BS:2 * BS], sides], axis=1)
            x_high = x.astype(jnp.bfloat16)
            x_low = (x - x_high.astype(jnp.float32)).astype(jnp.bfloat16)
            both = jnp.dot(x_high, taps, preferred_element_type=jnp.float32)
            y = both[:, :BS] + (both[:, BS:] + jnp.dot(
                x_low, taps[:, :BS], preferred_element_type=jnp.float32))
            y_high = y.astype(jnp.bfloat16)
            lanes = slice(half * BS, (half + 1) * BS)
            lines[0, :, lanes] = y_high
            lines[1, :, lanes] = (y - y_high.astype(jnp.float32)).astype(jnp.bfloat16)

    def along_rows(pair, acc):
        y_high, y_low = lines[0], lines[1]
        stacked = jnp.concatenate([y_high, y_low, y_high], axis=0)
        filtered = jnp.dot(wrow[...], stacked, preferred_element_type=jnp.float32)
        raised = lower + jnp.tanh(SHARPNESS * (filtered - THRESHOLD))
        for half in range(2):
            step = 2 * pair + half
            keep = meta_ref[layout.mask + meta_ref[begin + step]].astype(jnp.float32)
            value = raised[:, half * BS:(half + 1) * BS] * (keep * (1.0 / (lower + upper)))
            tiles[step] = value.astype(jnp.bfloat16)
            acc = acc + jnp.sum(value.reshape(BS // 8, 8, BS), axis=0)
        return acc

    def arrive(pair):
        slot = lax.rem(pair, BUFFERS)
        for half in range(2):
            pltpu.make_async_copy(dens.at[pl.ds(0, PAD), pl.ds(0, WIDE)],
                                  buf.at[slot, half], fetch_sem.at[slot, half]).wait()

    for ahead in range(min(BUFFERS - 1, pairs)):
        fetch(ahead, ahead)
    arrive(0)
    along_columns(0)

    def body(pair, acc):
        @pl.when(pair + BUFFERS - 2 < pairs)
        def _():
            fetch(pair + BUFFERS - 2, lax.rem(pair + BUFFERS - 2, BUFFERS))

        arrive(pair)
        acc = along_rows(pair - 1, acc)
        along_columns(pair)
        return acc

    acc = lax.fori_loop(1, pairs, body, acc_in[...])
    acc_out[...] = along_rows(pairs - 1, acc)

    stores = []
    for g in range(count):
        if has_local and g == count - 1:
            for r in range(capacity):
                slot = meta_ref[layout.place + (first + g) * capacity + r]
                stores.append(pltpu.make_async_copy(
                    tiles.at[g * capacity + r], outs[g].at[slot], store_sem.at[len(stores)]))
        else:
            stores.append(pltpu.make_async_copy(
                tiles.at[pl.ds(g * capacity, capacity)], outs[g], store_sem.at[len(stores)]))
    for store in stores:
        store.start()
    for store in stores:
        store.wait()


def project(meta, fields, acc, *, layout, first, count, block_rows, block_cols, has_local):
    capacity = layout.capacity
    block_count = block_rows * block_cols
    sent = jax.ShapeDtypeStruct((capacity, BS, BS), jnp.bfloat16)
    whole = jax.ShapeDtypeStruct((block_count, BS, BS), jnp.bfloat16)
    shapes = [sent] * count
    if has_local:
        shapes[-1] = whole
    anywhere = pl.BlockSpec(memory_space=pl.ANY)
    vmem = pl.BlockSpec(memory_space=pltpu.VMEM)
    kernel = functools.partial(
        project_kernel, layout=layout, first=first, count=count, block_rows=block_rows,
        block_cols=block_cols, has_local=has_local)
    steps = count * capacity
    results = pl.pallas_call(
        kernel,
        out_shape=tuple(shapes) + (jax.ShapeDtypeStruct((8, BS), jnp.float32),),
        in_specs=[pl.BlockSpec(memory_space=pltpu.SMEM)] + [anywhere] * 5 + [vmem] * 3,
        out_specs=tuple([anywhere] * count + [vmem]),
        scratch_shapes=[
            pltpu.VMEM((BUFFERS, 2, PAD, WIDE), jnp.float32),
            pltpu.SemaphoreType.DMA((BUFFERS, 2)),
            pltpu.VMEM((2, PAD, 2 * BS), jnp.bfloat16),
            pltpu.VMEM((steps, BS, BS), jnp.bfloat16),
            pltpu.SemaphoreType.DMA((count + capacity,)),
        ],
        cost_estimate=pl.CostEstimate(
            flops=steps * 300_000_000, bytes_accessed=steps * 300_000, transcendentals=0),
        name="project",
    )(meta, *fields, acc)
    return results[:-1], results[-1]


def place_kernel(meta_ref, out_in, *refs, layout, first, count, parts):
    del out_in
    arrived, refs = refs[:count], refs[count:]
    addends, refs = refs[:parts], refs[parts:]
    out, sem = refs[0], refs[-1]
    capacity = layout.capacity
    for g in range(count):
        for r in range(capacity):
            slot = meta_ref[layout.place + (first + g) * capacity + r]
            pltpu.make_async_copy(arrived[g].at[r], out.at[slot], sem).start()
    if parts:
        refs[1][...] = pairwise_sum([addend[...] for addend in addends])
    everything = out.at[pl.ds(0, count * capacity)]
    pltpu.make_async_copy(everything, everything, sem).wait()


def place(meta, out, arrived, addends, *, layout, first):
    anywhere = pl.BlockSpec(memory_space=pl.ANY)
    vmem = pl.BlockSpec(memory_space=pltpu.VMEM)
    shapes = [jax.ShapeDtypeStruct(out.shape, out.dtype)]
    shapes += [jax.ShapeDtypeStruct(a.shape, a.dtype) for a in addends[:1]]
    results = pl.pallas_call(
        functools.partial(place_kernel, layout=layout, first=first, count=len(arrived),
                          parts=len(addends)),
        out_shape=tuple(shapes),
        in_specs=[pl.BlockSpec(memory_space=pltpu.SMEM), anywhere]
        + [vmem] * (len(arrived) + len(addends)),
        out_specs=tuple([anywhere] + [vmem] * len(addends[:1])),
        scratch_shapes=[pltpu.SemaphoreType.DMA],
        input_output_aliases={1: 0},
        name="place",
    )(meta, out, *arrived, *addends)
    return results[0], results[-1]


def pairwise_sum(parts):
    while len(parts) > 1:
        parts = [a + b for a, b in zip(parts[::2], parts[1::2])]
    return parts[0]


def spread(value, axis):
    count = lax.axis_size(axis)
    parts = [value]
    for offset in range(1, count):
        parts.append(lax.ppermute(value, axis, [(i, i ^ offset) for i in range(count)]))
    return parts


def grouped(items, sizes):
    groups = []
    for size in sizes:
        if items:
            groups.append(items[:size])
            items = items[size:]
    return groups


def per_device(density, design_mask, rebalance):
    tile_rows, tile_cols = density.shape
    block_rows, block_cols = design_mask.shape
    block_count = block_rows * block_cols
    row_count = lax.axis_size("row")
    col_count = lax.axis_size("col")
    device_count = row_count * col_count
    capacity = block_count // device_count
    assert capacity * device_count == block_count and capacity % 2 == 0
    assert block_rows > 1 and block_cols > 1
    me = lax.axis_index(AXES)
    order = exchange_order(row_count, col_count) + [0]
    layout = Meta(device_count, capacity)
    top, bottom, left, right = with_halo(density)
    tables = block_tables(
        rebalance, me, block_rows, block_cols, row_count, col_count, capacity, order)
    meta = jnp.concatenate([tables, design_mask.reshape(-1)])
    fields = (density, top, bottom, left, right, *band_matrices())

    unit = max(1, 8 // capacity)
    groups = grouped(order, [unit * size for size in GROUPS])
    acc = jnp.zeros((8, BS), jnp.float32)
    arrivals, first = [], 0
    for group in groups:
        sent, acc = project(
            meta, fields, acc, layout=layout, first=first, count=len(group),
            block_rows=block_rows, block_cols=block_cols, has_local=group[-1] == 0)
        for offset, part in zip(group, sent):
            if offset:
                pairs = [(i, i ^ offset) for i in range(device_count)]
                arrivals.append(lax.ppermute(part, AXES, pairs))
            else:
                out = part
        first += len(group)

    tail = [2 * unit, 1 * unit]
    bulk = len(arrivals) - sum(tail)
    sizes = [bulk % (4 * unit)] + [4 * unit] * (bulk // (4 * unit)) + tail
    sizes = [size for size in sizes if size]
    begin = 0
    addends = spread(acc, "row")
    for index, size in enumerate(sizes):
        now = addends if index in (len(sizes) // 2, len(sizes) - 1) else []
        out, total = place(meta, out, arrivals[begin:begin + size], now,
                           layout=layout, first=begin)
        if index == len(sizes) // 2:
            addends = spread(total, "col")
        begin += size
    grid_cells = float(tile_rows * tile_cols * device_count)
    constraint = jnp.sum(total) / grid_cells / VOLUME_TARGET - 1.0
    return out, constraint


def solution(mesh):
    return jax.shard_map(
        per_device,
        mesh=mesh,
        in_specs=(P("row", "col"), P("row", "col"), P()),
        out_specs=(P(AXES, None, None), P()),
        check_vma=False,
    )
```

```python
import functools

import jax
import jax.numpy as jnp
import numpy as np
from jax import lax
from jax.experimental import pallas as pl
from jax.experimental.pallas import tpu as pltpu
from jax.sharding import PartitionSpec as P


BS = 128
RADIUS = 16
PAD = BS + 2 * RADIUS
WIDE = 3 * BS
BUFFERS = 4
ROW_SUM = 3
LEAD = 3
GROUPS = (1, 2, 4, 8, 8, 9)

SHARPNESS = 32.0
THRESHOLD = 0.5
VOLUME_TARGET = 0.4

AXES = ("row", "col")


def tap_parts():
    sigma = RADIUS / 4.0
    offsets = np.arange(2 * RADIUS + 1, dtype=np.float64) - RADIUS
    raw_taps = np.exp(-offsets * offsets / (2.0 * sigma * sigma))
    taps = raw_taps / raw_taps.sum()
    high = taps.astype(jnp.bfloat16)
    rest = taps - high.astype(np.float64)
    missing = (rest - rest.astype(jnp.bfloat16).astype(np.float64)).sum()
    rest[0] += missing / 2
    rest[-1] += missing / 2
    return high, rest.astype(jnp.bfloat16)


def band_matrices():
    parts = tap_parts()

    def bands(lag, used):
        used = used & (np.abs(lag) <= RADIUS)
        index = np.clip(lag + RADIUS, 0, 2 * RADIUS)
        return [np.where(used, part[index], np.zeros((), part.dtype)) for part in parts]

    lane = np.arange(2 * BS)[:, None]
    source = np.where(lane < 2 * BS - RADIUS, lane, lane - 2 * BS)
    used = (lane < BS + RADIUS) | (lane >= 2 * BS - RADIUS)
    columns = bands(source - np.arange(BS)[None, :], used)
    lag = np.arange(PAD)[None, :] - RADIUS - np.arange(BS)[:, None]
    rows = bands(lag, np.ones_like(lag, bool))
    return (jnp.asarray(np.concatenate(columns, axis=1)),
            jnp.asarray(np.concatenate([rows[0], rows[0], rows[1]], axis=1)))


def exchange_order(row_count, col_count):
    quarter = max(1, col_count // 4)
    rest = [r * col_count + c for r in range(row_count) for c in range(quarter)]
    middle = [part * quarter + other for other in rest for part in (2, 3)]
    light = []
    for other in rest:
        light += [quarter + other, other]
    light.reverse()
    order, middle = middle[:LEAD], middle[LEAD:]
    while middle or light:
        order += light[:2] + middle[:2]
        light, middle = light[2:], middle[2:]
    order = [d for d in order if d]
    assert sorted(order) == list(range(1, row_count * col_count))
    return order


def with_halo(density):
    rows, cols = density.shape

    def moves(axis):
        up = [(i, i + 1) for i in range(lax.axis_size(axis) - 1)]
        return up, [(j, i) for i, j in up]

    up, down = moves("row")
    top = lax.ppermute(density[rows - RADIUS:], "row", up)
    bottom = lax.ppermute(density[:RADIUS], "row", down)
    up, down = moves("col")

    def strip(start):
        parts = [a[:, start:start + RADIUS].T for a in (top, density, bottom)]
        return jnp.concatenate(parts, axis=1)

    left = lax.ppermute(strip(cols - RADIUS), "col", up)
    right = lax.ppermute(strip(0), "col", down)
    left = jnp.pad(left, ((BS - RADIUS, 0), (0, 0))).T
    right = jnp.pad(right, ((0, BS - RADIUS), (0, 0))).T
    return top, bottom, left, right


def block_tables(rebalance, me, mask_rows, mask_cols, row_count, col_count, capacity, order):
    device_count = row_count * col_count
    block_count = mask_rows * mask_cols
    wanted = rebalance.reshape(device_count, block_count)
    block_row = lax.div(wanted, mask_cols * col_count)
    block_col = lax.rem(wanted, mask_cols * col_count)
    source = lax.div(block_row, mask_rows) * col_count + lax.div(block_col, mask_cols)
    local = lax.rem(block_row, mask_rows) * mask_cols + lax.rem(block_col, mask_cols)
    slots = jnp.arange(block_count, dtype=jnp.int32)
    devices = jnp.arange(device_count, dtype=jnp.int32)
    mine = lax.dynamic_index_in_dim(source, me, 0, keepdims=True)
    match = jnp.concatenate([source == me, mine == devices[:, None]], axis=0)
    value = jnp.concatenate([local, jnp.broadcast_to(slots, local.shape)], axis=0)
    before = (slots[:, None] < slots[None, :]).astype(jnp.bfloat16)
    rank = jnp.dot(match.astype(jnp.bfloat16), before, preferred_element_type=jnp.float32)
    rank = jnp.where(match, rank.astype(jnp.int32), -1)
    ranks = jnp.arange(capacity, dtype=jnp.int32)
    chosen = rank[:, None, :] == ranks[None, :, None]
    table = jnp.sum(jnp.where(chosen, value[:, None, :], 0), axis=2)
    partner = me ^ jnp.array(order, jnp.int32)
    pick = partner[:, None] == devices[None, :]
    table = table.reshape(2, 1, device_count, capacity)
    return jnp.sum(jnp.where(pick[None, :, :, None], table, 0), axis=2).reshape(-1)


class Meta:
    def __init__(self, device_count, capacity):
        self.capacity = capacity
        self.send = 0
        self.place = device_count * capacity
        self.mask = 2 * device_count * capacity


def split_scalar(index, size):
    if size & (size - 1):
        return lax.div(index, size), lax.rem(index, size)
    return lax.shift_right_logical(index, size.bit_length() - 1), index & (size - 1)


def project_kernel(meta_ref, dens, top, bottom, left, right, wcol, wrow, acc_in, *refs,
                   layout, first, count, block_rows, block_cols, has_local):
    capacity = layout.capacity
    outs, acc_out = refs[:count], refs[count]
    buf, fetch_sem, lines, tiles, store_sem = refs[count + 1:]
    pairs = count * capacity // 2
    begin = layout.send + first * capacity

    def fetch(pair, slot):
        for half in range(2):
            block = meta_ref[begin + 2 * pair + half]
            br, bc = split_scalar(block, block_cols)
            row0 = pl.multiple_of(br * BS, BS)
            col0 = pl.multiple_of(bc * BS, BS)
            window = buf.at[slot, half]
            sem = fetch_sem.at[slot, half]
            inside = ((br > 0) & (br < block_rows - 1)) & ((bc > 0) & (bc < block_cols - 1))

            def copy(src, rows, cols):
                pltpu.make_async_copy(src, window.at[pl.ds(*rows), pl.ds(*cols)], sem).start()

            def rows_of(span, c_dst, c_len):
                @pl.when(br == 0)
                def _():
                    copy(top.at[:, span], (0, RADIUS), (c_dst, c_len))
                    copy(dens.at[pl.ds(0, PAD - RADIUS), span],
                         (RADIUS, PAD - RADIUS), (c_dst, c_len))

                @pl.when((br > 0) & (br < block_rows - 1))
                def _():
                    row1 = pl.multiple_of(row0 - RADIUS, RADIUS)
                    copy(dens.at[pl.ds(row1, PAD), span], (0, PAD), (c_dst, c_len))

                @pl.when(br == block_rows - 1)
                def _():
                    last = block_rows * BS - (PAD - RADIUS)
                    copy(dens.at[pl.ds(last, PAD - RADIUS), span],
                         (0, PAD - RADIUS), (c_dst, c_len))
                    copy(bottom.at[:, span], (PAD - RADIUS, RADIUS), (c_dst, c_len))

            @pl.when(inside)
            def _():
                row1 = pl.multiple_of(row0 - RADIUS, RADIUS)
                col1 = pl.multiple_of(col0 - BS, BS)
                pltpu.make_async_copy(
                    dens.at[pl.ds(row1, PAD), pl.ds(col1, WIDE)], window, sem).start()

            @pl.when(jnp.logical_not(inside))
            def _():
                @pl.when(bc == 0)
                def _():
                    copy(left.at[pl.ds(row0, PAD), :], (0, PAD), (0, BS))
                    rows_of(pl.ds(0, 2 * BS), BS, 2 * BS)

                @pl.when((bc > 0) & (bc < block_cols - 1))
                def _():
                    rows_of(pl.ds(pl.multiple_of(col0 - BS, BS), WIDE), 0, WIDE)

                @pl.when(bc == block_cols - 1)
                def _():
                    copy(right.at[pl.ds(row0, PAD), :], (0, PAD), (2 * BS, BS))
                    rows_of(pl.ds((block_cols - 2) * BS, 2 * BS), 0, 2 * BS)

    lower = float(np.tanh(SHARPNESS * THRESHOLD))
    upper = float(np.tanh(SHARPNESS * (1.0 - THRESHOLD)))

    def along_columns(pair):
        slot = lax.rem(pair, BUFFERS)
        lane = lax.broadcasted_iota(jnp.int32, (PAD, BS), 1)
        taps = wcol[...]
        for half in range(2):
            window = buf.at[slot, half]
            sides = jnp.where(lane < BS // 2, window[:, 2 * BS:], window[:, :BS])
            x = jnp.concatenate([window[:, BS:2 * BS], sides], axis=1)
            x_high = x.astype(jnp.bfloat16)
            x_low = (x - x_high.astype(jnp.float32)).astype(jnp.bfloat16)
            both = jnp.dot(x_high, taps, preferred_element_type=jnp.float32)
            y = both[:, :BS] + (both[:, BS:] + jnp.dot(
                x_low, taps[:, :BS], preferred_element_type=jnp.float32))
            y_high = y.astype(jnp.bfloat16)
            lanes = slice(half * BS, (half + 1) * BS)
            lines[0, :, lanes] = y_high
            lines[1, :, lanes] = (y - y_high.astype(jnp.float32)).astype(jnp.bfloat16)

    def along_rows(pair, acc):
        y_high, y_low = lines[0], lines[1]
        stacked = jnp.concatenate([y_high, y_low, y_high], axis=0)
        filtered = jnp.dot(wrow[...], stacked, preferred_element_type=jnp.float32)
        raised = lower + jnp.tanh(SHARPNESS * (filtered - THRESHOLD))
        for half in range(2):
            step = 2 * pair + half
            keep = meta_ref[layout.mask + meta_ref[begin + step]].astype(jnp.float32)
            value = raised[:, half * BS:(half + 1) * BS] * (keep * (1.0 / (lower + upper)))
            tiles[step] = value.astype(jnp.bfloat16)
            acc = acc + jnp.sum(value.reshape(BS // 8, 8, BS), axis=0)
        return acc

    def arrive(pair):
        slot = lax.rem(pair, BUFFERS)
        for half in range(2):
            pltpu.make_async_copy(dens.at[pl.ds(0, PAD), pl.ds(0, WIDE)],
                                  buf.at[slot, half], fetch_sem.at[slot, half]).wait()

    for ahead in range(min(BUFFERS - 1, pairs)):
        fetch(ahead, ahead)
    arrive(0)
    along_columns(0)

    def body(pair, acc):
        @pl.when(pair + BUFFERS - 2 < pairs)
        def _():
            fetch(pair + BUFFERS - 2, lax.rem(pair + BUFFERS - 2, BUFFERS))

        arrive(pair)
        acc = along_rows(pair - 1, acc)
        along_columns(pair)
        return acc

    acc = lax.fori_loop(1, pairs, body, acc_in[...])
    acc_out[...] = along_rows(pairs - 1, acc)

    stores = []
    for g in range(count):
        if has_local and g == count - 1:
            for r in range(capacity):
                slot = meta_ref[layout.place + (first + g) * capacity + r]
                stores.append(pltpu.make_async_copy(
                    tiles.at[g * capacity + r], outs[g].at[slot], store_sem.at[len(stores)]))
        else:
            stores.append(pltpu.make_async_copy(
                tiles.at[pl.ds(g * capacity, capacity)], outs[g], store_sem.at[len(stores)]))
    for store in stores:
        store.start()
    for store in stores:
        store.wait()


def project(meta, fields, acc, *, layout, first, count, block_rows, block_cols, has_local):
    capacity = layout.capacity
    block_count = block_rows * block_cols
    sent = jax.ShapeDtypeStruct((capacity, BS, BS), jnp.bfloat16)
    whole = jax.ShapeDtypeStruct((block_count, BS, BS), jnp.bfloat16)
    shapes = [sent] * count
    if has_local:
        shapes[-1] = whole
    anywhere = pl.BlockSpec(memory_space=pl.ANY)
    vmem = pl.BlockSpec(memory_space=pltpu.VMEM)
    kernel = functools.partial(
        project_kernel, layout=layout, first=first, count=count, block_rows=block_rows,
        block_cols=block_cols, has_local=has_local)
    steps = count * capacity
    results = pl.pallas_call(
        kernel,
        out_shape=tuple(shapes) + (jax.ShapeDtypeStruct((8, BS), jnp.float32),),
        in_specs=[pl.BlockSpec(memory_space=pltpu.SMEM)] + [anywhere] * 5 + [vmem] * 3,
        out_specs=tuple([anywhere] * count + [vmem]),
        scratch_shapes=[
            pltpu.VMEM((BUFFERS, 2, PAD, WIDE), jnp.float32),
            pltpu.SemaphoreType.DMA((BUFFERS, 2)),
            pltpu.VMEM((2, PAD, 2 * BS), jnp.bfloat16),
            pltpu.VMEM((steps, BS, BS), jnp.bfloat16),
            pltpu.SemaphoreType.DMA((count + capacity,)),
        ],
        cost_estimate=pl.CostEstimate(
            flops=steps * 300_000_000, bytes_accessed=steps * 300_000, transcendentals=0),
        name="project",
    )(meta, *fields, acc)
    return results[:-1], results[-1]


def place_kernel(meta_ref, out_in, *refs, layout, first, count, parts, finish):
    del out_in
    arrived, refs = refs[:count], refs[count:]
    addends, refs = refs[:parts], refs[parts:]
    out, sem = refs[0], refs[-1]
    capacity = layout.capacity
    for g in range(count):
        for r in range(capacity):
            slot = meta_ref[layout.place + (first + g) * capacity + r]
            pltpu.make_async_copy(arrived[g].at[r], out.at[slot], sem).start()
    if parts:
        total = pairwise_sum([addend[...] for addend in addends])
        refs[1][...] = finish(total) if finish else total
    everything = out.at[pl.ds(0, count * capacity)]
    pltpu.make_async_copy(everything, everything, sem).wait()


def place(meta, out, arrived, addends, *, layout, first, finish=None):
    anywhere = pl.BlockSpec(memory_space=pl.ANY)
    vmem = pl.BlockSpec(memory_space=pltpu.VMEM)
    shapes = [jax.ShapeDtypeStruct(out.shape, out.dtype)]
    shapes += [jax.ShapeDtypeStruct((1, 1) if finish else a.shape, a.dtype)
               for a in addends[:1]]
    results = pl.pallas_call(
        functools.partial(place_kernel, layout=layout, first=first, count=len(arrived),
                          parts=len(addends), finish=finish),
        out_shape=tuple(shapes),
        in_specs=[pl.BlockSpec(memory_space=pltpu.SMEM), anywhere]
        + [vmem] * (len(arrived) + len(addends)),
        out_specs=tuple([anywhere] + [vmem] * len(addends[:1])),
        scratch_shapes=[pltpu.SemaphoreType.DMA],
        input_output_aliases={1: 0},
        name="place",
    )(meta, out, *arrived, *addends)
    return results[0], results[-1]


def pairwise_sum(parts):
    while len(parts) > 1:
        parts = [a + b for a, b in zip(parts[::2], parts[1::2])]
    return parts[0]


def spread(value, axis):
    count = lax.axis_size(axis)
    parts = [value]
    for offset in range(1, count):
        part = lax.ppermute(value, axis, [(i, i ^ offset) for i in range(count)])
        parts.append(pltpu.with_memory_space_constraint(part, pltpu.VMEM))
    return parts


def grouped(items, sizes):
    groups = []
    for size in sizes:
        if items:
            groups.append(items[:size])
            items = items[size:]
    return groups


def per_device(density, design_mask, rebalance):
    tile_rows, tile_cols = density.shape
    block_rows, block_cols = design_mask.shape
    block_count = block_rows * block_cols
    row_count = lax.axis_size("row")
    col_count = lax.axis_size("col")
    device_count = row_count * col_count
    capacity = block_count // device_count
    assert capacity * device_count == block_count and capacity % 2 == 0
    assert block_rows > 1 and block_cols > 1
    me = lax.axis_index(AXES)
    order = exchange_order(row_count, col_count) + [0]
    layout = Meta(device_count, capacity)
    top, bottom, left, right = with_halo(density)
    tables = block_tables(
        rebalance, me, block_rows, block_cols, row_count, col_count, capacity, order)
    meta = jnp.concatenate([tables, design_mask.reshape(-1)])
    fields = (density, top, bottom, left, right, *band_matrices())

    unit = max(1, 8 // capacity)
    groups = grouped(order, [unit * size for size in GROUPS])
    acc = jnp.zeros((8, BS), jnp.float32)
    arrivals, first = [], 0
    for group in groups:
        sent, acc = project(
            meta, fields, acc, layout=layout, first=first, count=len(group),
            block_rows=block_rows, block_cols=block_cols, has_local=group[-1] == 0)
        for offset, part in zip(group, sent):
            if offset:
                pairs = [(i, i ^ offset) for i in range(device_count)]
                part = lax.ppermute(part, AXES, pairs)
                arrivals.append(pltpu.with_memory_space_constraint(part, pltpu.VMEM))
            else:
                out = part
        first += len(group)

    tail = [2 * unit, 1 * unit]
    bulk = len(arrivals) - sum(tail)
    sizes = [bulk % (4 * unit)] + [4 * unit] * (bulk // (4 * unit)) + tail
    sizes = [size for size in sizes if size]
    grid_cells = float(tile_rows * tile_cols * device_count)

    def constraint_of(total):
        volume = jnp.sum(jnp.sum(total, axis=0, keepdims=True), axis=1, keepdims=True)
        return volume / grid_cells / VOLUME_TARGET - 1.0

    begin = 0
    addends = spread(acc, "row")
    for index, size in enumerate(sizes):
        last = index == len(sizes) - 1
        out, total = place(meta, out, arrivals[begin:begin + size],
                           addends if last or index == ROW_SUM else [],
                           layout=layout, first=begin, finish=constraint_of if last else None)
        if index == ROW_SUM:
            addends = spread(total, "col")
        begin += size
    return out, total.reshape(())


def solution(mesh):
    return jax.shard_map(
        per_device,
        mesh=mesh,
        in_specs=(P("row", "col"), P("row", "col"), P()),
        out_specs=(P(AXES, None, None), P()),
        check_vma=False,
    )
```

```python
import functools

import jax
import jax.numpy as jnp
import numpy as np
from jax import lax
from jax.experimental import pallas as pl
from jax.experimental.pallas import tpu as pltpu
from jax.sharding import PartitionSpec as P


BS = 128
RADIUS = 16
PAD = BS + 2 * RADIUS
WIDE = 3 * BS
BUFFERS = 4
ROW_SUM = 3
LEAD = 3
GROUPS = (1, 2, 4, 8, 8, 9)

SHARPNESS = 32.0
THRESHOLD = 0.5
VOLUME_TARGET = 0.4

AXES = ("row", "col")


def tap_parts():
    sigma = RADIUS / 4.0
    offsets = np.arange(2 * RADIUS + 1, dtype=np.float64) - RADIUS
    raw_taps = np.exp(-offsets * offsets / (2.0 * sigma * sigma))
    taps = raw_taps / raw_taps.sum()
    high = taps.astype(jnp.bfloat16)
    rest = taps - high.astype(np.float64)
    missing = (rest - rest.astype(jnp.bfloat16).astype(np.float64)).sum()
    rest[0] += missing / 2
    rest[-1] += missing / 2
    return high, rest.astype(jnp.bfloat16)


def band_matrices():
    parts = tap_parts()

    def bands(lag, used):
        used = used & (np.abs(lag) <= RADIUS)
        index = np.clip(lag + RADIUS, 0, 2 * RADIUS)
        return [np.where(used, part[index], np.zeros((), part.dtype)) for part in parts]

    lane = np.arange(2 * BS)[:, None]
    source = np.where(lane < 2 * BS - RADIUS, lane, lane - 2 * BS)
    used = (lane < BS + RADIUS) | (lane >= 2 * BS - RADIUS)
    columns = bands(source - np.arange(BS)[None, :], used)
    lag = np.arange(PAD)[None, :] - RADIUS - np.arange(BS)[:, None]
    rows = bands(lag, np.ones_like(lag, bool))
    return (jnp.asarray(np.concatenate(columns, axis=1)),
            jnp.asarray(np.concatenate([rows[0], rows[0], rows[1]], axis=1)))


def exchange_order(row_count, col_count):
    quarter = max(1, col_count // 4)
    rest = [r * col_count + c for r in range(row_count) for c in range(quarter)]
    middle = [part * quarter + other for other in rest for part in (2, 3)]
    light = []
    for other in rest:
        light += [quarter + other, other]
    light.reverse()
    order, middle = middle[:LEAD], middle[LEAD:]
    while middle or light:
        order += light[:2] + middle[:2]
        light, middle = light[2:], middle[2:]
    order = [d for d in order if d]
    assert sorted(order) == list(range(1, row_count * col_count))
    return order


def with_halo(density):
    rows, cols = density.shape

    def moves(axis):
        up = [(i, i + 1) for i in range(lax.axis_size(axis) - 1)]
        return up, [(j, i) for i, j in up]

    up, down = moves("row")
    top = lax.ppermute(density[rows - RADIUS:], "row", up)
    bottom = lax.ppermute(density[:RADIUS], "row", down)
    up, down = moves("col")

    def strip(start):
        parts = [a[:, start:start + RADIUS].T for a in (top, density, bottom)]
        return jnp.concatenate(parts, axis=1)

    left = lax.ppermute(strip(cols - RADIUS), "col", up)
    right = lax.ppermute(strip(0), "col", down)
    left = jnp.pad(left, ((BS - RADIUS, 0), (0, 0))).T
    right = jnp.pad(right, ((0, BS - RADIUS), (0, 0))).T
    return top, bottom, left, right


def block_tables(rebalance, me, mask_rows, mask_cols, row_count, col_count, capacity, order):
    device_count = row_count * col_count
    block_count = mask_rows * mask_cols
    wanted = rebalance.reshape(device_count, block_count)
    block_row = lax.div(wanted, mask_cols * col_count)
    block_col = lax.rem(wanted, mask_cols * col_count)
    source = lax.div(block_row, mask_rows) * col_count + lax.div(block_col, mask_cols)
    local = lax.rem(block_row, mask_rows) * mask_cols + lax.rem(block_col, mask_cols)
    slots = jnp.arange(block_count, dtype=jnp.int32)
    devices = jnp.arange(device_count, dtype=jnp.int32)
    mine = lax.dynamic_index_in_dim(source, me, 0, keepdims=True)
    match = jnp.concatenate([source == me, mine == devices[:, None]], axis=0)
    value = jnp.concatenate([local, jnp.broadcast_to(slots, local.shape)], axis=0)
    before = (slots[:, None] < slots[None, :]).astype(jnp.bfloat16)
    rank = jnp.dot(match.astype(jnp.bfloat16), before, preferred_element_type=jnp.float32)
    rank = jnp.where(match, rank.astype(jnp.int32), -1)
    ranks = jnp.arange(capacity, dtype=jnp.int32)
    chosen = rank[:, None, :] == ranks[None, :, None]
    table = jnp.sum(jnp.where(chosen, value[:, None, :], 0), axis=2)
    partner = me ^ jnp.array(order, jnp.int32)
    pick = partner[:, None] == devices[None, :]
    table = table.reshape(2, 1, device_count, capacity)
    return jnp.sum(jnp.where(pick[None, :, :, None], table, 0), axis=2).reshape(-1)


class Meta:
    def __init__(self, device_count, capacity):
        self.capacity = capacity
        self.send = 0
        self.place = device_count * capacity
        self.mask = 2 * device_count * capacity


def split_scalar(index, size):
    if size & (size - 1):
        return lax.div(index, size), lax.rem(index, size)
    return lax.shift_right_logical(index, size.bit_length() - 1), index & (size - 1)


def project_kernel(meta_ref, dens, top, bottom, left, right, wcol, wrow, *refs,
                   layout, first, count, block_rows, block_cols, has_local):
    capacity = layout.capacity
    if first:
        acc = refs[0][...]
        refs = refs[1:]
    else:
        acc = jnp.zeros((8, BS), jnp.float32)
    outs, acc_out = refs[:count], refs[count]
    buf, fetch_sem, lines, tiles, store_sem = refs[count + 1:]
    pairs = count * capacity // 2
    begin = layout.send + first * capacity

    def fetch(pair, slot):
        for half in range(2):
            block = meta_ref[begin + 2 * pair + half]
            br, bc = split_scalar(block, block_cols)
            row0 = pl.multiple_of(br * BS, BS)
            col0 = pl.multiple_of(bc * BS, BS)
            window = buf.at[slot, half]
            sem = fetch_sem.at[slot, half]
            inside = ((br > 0) & (br < block_rows - 1)) & ((bc > 0) & (bc < block_cols - 1))

            def copy(src, rows, cols):
                pltpu.make_async_copy(src, window.at[pl.ds(*rows), pl.ds(*cols)], sem).start()

            def rows_of(span, c_dst, c_len):
                @pl.when(br == 0)
                def _():
                    copy(top.at[:, span], (0, RADIUS), (c_dst, c_len))
                    copy(dens.at[pl.ds(0, PAD - RADIUS), span],
                         (RADIUS, PAD - RADIUS), (c_dst, c_len))

                @pl.when((br > 0) & (br < block_rows - 1))
                def _():
                    row1 = pl.multiple_of(row0 - RADIUS, RADIUS)
                    copy(dens.at[pl.ds(row1, PAD), span], (0, PAD), (c_dst, c_len))

                @pl.when(br == block_rows - 1)
                def _():
                    last = block_rows * BS - (PAD - RADIUS)
                    copy(dens.at[pl.ds(last, PAD - RADIUS), span],
                         (0, PAD - RADIUS), (c_dst, c_len))
                    copy(bottom.at[:, span], (PAD - RADIUS, RADIUS), (c_dst, c_len))

            @pl.when(inside)
            def _():
                row1 = pl.multiple_of(row0 - RADIUS, RADIUS)
                col1 = pl.multiple_of(col0 - BS, BS)
                pltpu.make_async_copy(
                    dens.at[pl.ds(row1, PAD), pl.ds(col1, WIDE)], window, sem).start()

            @pl.when(jnp.logical_not(inside))
            def _():
                @pl.when(bc == 0)
                def _():
                    copy(left.at[pl.ds(row0, PAD), :], (0, PAD), (0, BS))
                    rows_of(pl.ds(0, 2 * BS), BS, 2 * BS)

                @pl.when((bc > 0) & (bc < block_cols - 1))
                def _():
                    rows_of(pl.ds(pl.multiple_of(col0 - BS, BS), WIDE), 0, WIDE)

                @pl.when(bc == block_cols - 1)
                def _():
                    copy(right.at[pl.ds(row0, PAD), :], (0, PAD), (2 * BS, BS))
                    rows_of(pl.ds((block_cols - 2) * BS, 2 * BS), 0, 2 * BS)

    lower = float(np.tanh(SHARPNESS * THRESHOLD))
    upper = float(np.tanh(SHARPNESS * (1.0 - THRESHOLD)))

    def along_columns(pair):
        slot = lax.rem(pair, BUFFERS)
        lane = lax.broadcasted_iota(jnp.int32, (PAD, BS), 1)
        taps = wcol[...]
        for half in range(2):
            window = buf.at[slot, half]
            sides = jnp.where(lane < BS // 2, window[:, 2 * BS:], window[:, :BS])
            x = jnp.concatenate([window[:, BS:2 * BS], sides], axis=1)
            x_high = x.astype(jnp.bfloat16)
            x_low = (x - x_high.astype(jnp.float32)).astype(jnp.bfloat16)
            both = jnp.dot(x_high, taps, preferred_element_type=jnp.float32)
            y = both[:, :BS] + (both[:, BS:] + jnp.dot(
                x_low, taps[:, :BS], preferred_element_type=jnp.float32))
            y_high = y.astype(jnp.bfloat16)
            lanes = slice(half * BS, (half + 1) * BS)
            lines[0, :, lanes] = y_high
            lines[1, :, lanes] = (y - y_high.astype(jnp.float32)).astype(jnp.bfloat16)

    def along_rows(pair, acc):
        y_high, y_low = lines[0], lines[1]
        stacked = jnp.concatenate([y_high, y_low, y_high], axis=0)
        filtered = jnp.dot(wrow[...], stacked, preferred_element_type=jnp.float32)
        raised = lower + jnp.tanh(SHARPNESS * (filtered - THRESHOLD))
        for half in range(2):
            step = 2 * pair + half
            keep = meta_ref[layout.mask + meta_ref[begin + step]].astype(jnp.float32)
            value = raised[:, half * BS:(half + 1) * BS] * (keep * (1.0 / (lower + upper)))
            tiles[step] = value.astype(jnp.bfloat16)
            acc = acc + jnp.sum(value.reshape(BS // 8, 8, BS), axis=0)
        return acc

    def arrive(pair):
        slot = lax.rem(pair, BUFFERS)
        for half in range(2):
            pltpu.make_async_copy(dens.at[pl.ds(0, PAD), pl.ds(0, WIDE)],
                                  buf.at[slot, half], fetch_sem.at[slot, half]).wait()

    for ahead in range(min(BUFFERS - 1, pairs)):
        fetch(ahead, ahead)
    arrive(0)
    along_columns(0)

    def body(pair, acc):
        @pl.when(pair + BUFFERS - 2 < pairs)
        def _():
            fetch(pair + BUFFERS - 2, lax.rem(pair + BUFFERS - 2, BUFFERS))

        arrive(pair)
        acc = along_rows(pair - 1, acc)
        along_columns(pair)
        return acc

    acc = lax.fori_loop(1, pairs, body, acc)
    acc_out[...] = along_rows(pairs - 1, acc)

    stores = []
    for g in range(count):
        if has_local and g == count - 1:
            for r in range(capacity):
                slot = meta_ref[layout.place + (first + g) * capacity + r]
                stores.append(pltpu.make_async_copy(
                    tiles.at[g * capacity + r], outs[g].at[slot], store_sem.at[len(stores)]))
        else:
            stores.append(pltpu.make_async_copy(
                tiles.at[pl.ds(g * capacity, capacity)], outs[g], store_sem.at[len(stores)]))
    for store in stores:
        store.start()
    for store in stores:
        store.wait()


def project(meta, fields, acc, *, layout, first, count, block_rows, block_cols, has_local):
    capacity = layout.capacity
    block_count = block_rows * block_cols
    sent = jax.ShapeDtypeStruct((capacity, BS, BS), jnp.bfloat16)
    whole = jax.ShapeDtypeStruct((block_count, BS, BS), jnp.bfloat16)
    shapes = [sent] * count
    if has_local:
        shapes[-1] = whole
    anywhere = pl.BlockSpec(memory_space=pl.ANY)
    vmem = pl.BlockSpec(memory_space=pltpu.VMEM)
    kernel = functools.partial(
        project_kernel, layout=layout, first=first, count=count, block_rows=block_rows,
        block_cols=block_cols, has_local=has_local)
    steps = count * capacity
    results = pl.pallas_call(
        kernel,
        out_shape=tuple(shapes) + (jax.ShapeDtypeStruct((8, BS), jnp.float32),),
        in_specs=[pl.BlockSpec(memory_space=pltpu.SMEM)] + [anywhere] * 5
        + [vmem] * (2 + len(acc)),
        out_specs=tuple([anywhere] * count + [vmem]),
        scratch_shapes=[
            pltpu.VMEM((BUFFERS, 2, PAD, WIDE), jnp.float32),
            pltpu.SemaphoreType.DMA((BUFFERS, 2)),
            pltpu.VMEM((2, PAD, 2 * BS), jnp.bfloat16),
            pltpu.VMEM((steps, BS, BS), jnp.bfloat16),
            pltpu.SemaphoreType.DMA((count + capacity,)),
        ],
        cost_estimate=pl.CostEstimate(
            flops=steps * 300_000_000, bytes_accessed=steps * 300_000, transcendentals=0),
        name="project",
    )(meta, *fields, *acc)
    return results[:-1], results[-1]


def place_kernel(meta_ref, out_in, *refs, layout, first, count, parts, finish):
    del out_in
    arrived, refs = refs[:count], refs[count:]
    addends, refs = refs[:parts], refs[parts:]
    out, sem = refs[0], refs[-1]
    capacity = layout.capacity
    for g in range(count):
        for r in range(capacity):
            slot = meta_ref[layout.place + (first + g) * capacity + r]
            pltpu.make_async_copy(arrived[g].at[r], out.at[slot], sem).start()
    if parts:
        total = pairwise_sum([addend[...] for addend in addends])
        refs[1][...] = finish(total) if finish else total
    everything = out.at[pl.ds(0, count * capacity)]
    pltpu.make_async_copy(everything, everything, sem).wait()


def place(meta, out, arrived, addends, *, layout, first, finish=None):
    anywhere = pl.BlockSpec(memory_space=pl.ANY)
    vmem = pl.BlockSpec(memory_space=pltpu.VMEM)
    shapes = [jax.ShapeDtypeStruct(out.shape, out.dtype)]
    shapes += [jax.ShapeDtypeStruct((1, 1) if finish else a.shape, a.dtype)
               for a in addends[:1]]
    results = pl.pallas_call(
        functools.partial(place_kernel, layout=layout, first=first, count=len(arrived),
                          parts=len(addends), finish=finish),
        out_shape=tuple(shapes),
        in_specs=[pl.BlockSpec(memory_space=pltpu.SMEM), anywhere]
        + [vmem] * (len(arrived) + len(addends)),
        out_specs=tuple([anywhere] + [vmem] * len(addends[:1])),
        scratch_shapes=[pltpu.SemaphoreType.DMA],
        input_output_aliases={1: 0},
        name="place",
    )(meta, out, *arrived, *addends)
    return results[0], results[-1]


def pairwise_sum(parts):
    while len(parts) > 1:
        parts = [a + b for a, b in zip(parts[::2], parts[1::2])]
    return parts[0]


def spread(value, axis):
    count = lax.axis_size(axis)
    parts = [value]
    for offset in range(1, count):
        part = lax.ppermute(value, axis, [(i, i ^ offset) for i in range(count)])
        parts.append(pltpu.with_memory_space_constraint(part, pltpu.VMEM))
    return parts


def grouped(items, sizes):
    groups = []
    for size in sizes:
        if items:
            groups.append(items[:size])
            items = items[size:]
    return groups


def per_device(density, design_mask, rebalance):
    tile_rows, tile_cols = density.shape
    block_rows, block_cols = design_mask.shape
    block_count = block_rows * block_cols
    row_count = lax.axis_size("row")
    col_count = lax.axis_size("col")
    device_count = row_count * col_count
    capacity = block_count // device_count
    assert capacity * device_count == block_count and capacity % 2 == 0
    assert block_rows > 1 and block_cols > 1
    me = lax.axis_index(AXES)
    order = exchange_order(row_count, col_count) + [0]
    layout = Meta(device_count, capacity)
    top, bottom, left, right = with_halo(density)
    tables = block_tables(
        rebalance, me, block_rows, block_cols, row_count, col_count, capacity, order)
    meta = jnp.concatenate([tables, design_mask.reshape(-1)])
    fields = (density, top, bottom, left, right, *band_matrices())

    unit = max(1, 8 // capacity)
    groups = grouped(order, [unit * size for size in GROUPS])
    acc = None
    arrivals, first = [], 0
    for group in groups:
        sent, acc = project(
            meta, fields, () if acc is None else (acc,), layout=layout, first=first, count=len(group),
            block_rows=block_rows, block_cols=block_cols, has_local=group[-1] == 0)
        for offset, part in zip(group, sent):
            if offset:
                pairs = [(i, i ^ offset) for i in range(device_count)]
                part = lax.ppermute(part, AXES, pairs)
                arrivals.append(pltpu.with_memory_space_constraint(part, pltpu.VMEM))
            else:
                out = part
        first += len(group)

    tail = [2 * unit, 1 * unit]
    bulk = len(arrivals) - sum(tail)
    sizes = [bulk % (4 * unit)] + [4 * unit] * (bulk // (4 * unit)) + tail
    sizes = [size for size in sizes if size]
    grid_cells = float(tile_rows * tile_cols * device_count)

    def constraint_of(total):
        volume = jnp.sum(jnp.sum(total, axis=0, keepdims=True), axis=1, keepdims=True)
        return volume / grid_cells / VOLUME_TARGET - 1.0

    begin = 0
    addends = spread(acc, "row")
    for index, size in enumerate(sizes):
        last = index == len(sizes) - 1
        out, total = place(meta, out, arrivals[begin:begin + size],
                           addends if last or index == ROW_SUM else [],
                           layout=layout, first=begin, finish=constraint_of if last else None)
        if index == ROW_SUM:
            addends = spread(total, "col")
        begin += size
    return out, total.reshape(())


def solution(mesh):
    return jax.shard_map(
        per_device,
        mesh=mesh,
        in_specs=(P("row", "col"), P("row", "col"), P()),
        out_specs=(P(AXES, None, None), P()),
        check_vma=False,
    )
```
